256 devices in a mesh: group: 2 (over y), expert: 32 (over z, core), tensor: 4 (over x).
Axes of the slice: x: 4, y: 2, z: 16, core: 2. Of those that a mesh axis runs over, the one named last changes fastest.
The devices are a block of a 4x16x16 slice.
Arguments:
- tokens: bfloat16 [16384, 4096], P(('group', 'expert', 'tensor')), parts along dimension 0, may hold values from -6 to 6
- cotangent: bfloat16 [16384, 4096], P(('group', 'expert', 'tensor')), parts along dimension 0, may hold values from -6 to 6
- expert_ids: int32 [16384, 2], P(('group', 'expert', 'tensor')), parts along dimension 0, may hold values from 0 to 31, all different within a row
- gate_wts: float32 [16384, 2], P(('group', 'expert', 'tensor')), parts along dimension 0, may hold values from 0.2 to 1
- w_gate: bfloat16 [32, 4096, 256], P('expert', 'tensor'), may hold values from -0.09375 to 0.09375
- w_up: bfloat16 [32, 4096, 256], P('expert', 'tensor'), may hold values from -0.09375 to 0.09375
- w_down: bfloat16 [32, 256, 4096], P('expert', 'tensor'), may hold values from -0.375 to 0.375
Outputs:
- input_grad: bfloat16 [16384, 4096], P(('group', 'expert', 'tensor')), parts along dimension 0
- grad_gate: bfloat16 [64, 4096, 256], P(('group', 'expert'), 'tensor'), parts along dimension 0
- grad_up: bfloat16 [64, 4096, 256], P(('group', 'expert'), 'tensor'), parts along dimension 0
- grad_down: bfloat16 [64, 256, 4096], P(('group', 'expert'), 'tensor'), parts along dimension 0
The draws below stay inside these ranges and needn't reach their ends.
There are 2 independent parts, one for each index of `group`. The reference program is written for one: setup_inputs(seed, part) draws one part's arguments, and reference() takes and returns one part's arrays. A program takes and returns all parts, laid end to end along the dimension named above; an argument that names none is the same for every part. Nothing has to cross between parts.
Inputs may be any that keep to these rules, and one draw needn't show every extreme that they name: `expert_ids`: the two ids of a token differ.
All inputs are finite; a program needn't handle non-finite values.
Results may differ from the reference program's by a relative error of at most 0.009.
Values may be sent and summed in bfloat16 or wider, within the bound.
A program may use at most 64 MiB of HBM per device.

```python
import jax
import jax.numpy as jnp
from jax import lax

D = 4096
FF = 256
TOK_DEV = 64
EXPERTS = 32
CAP = 4
TOKENS = 8192
N_EXPERT = 32
N_TENSOR = 4


def block_levels(key, shape, pieces, least, top_value):
    factor_of, own = 1.0, jax.random.fold_in(key, 6)
    for position, blocks in pieces:
        steps = jnp.exp(jax.random.uniform(jax.random.fold_in(own, position), (blocks,), jnp.float32, least / len(pieces), top_value / len(pieces)))
        factor_of = factor_of * jnp.repeat(steps, shape[position] // blocks).reshape([-1 if axis == position else 1 for axis in range(len(shape))])
    return factor_of


def different_ones(key, rows, amount, top, lift):
    ranking = jax.random.permutation(jax.random.fold_in(key, 1), amount)
    pull = ranking
    for power in range(3):
        pull = pull * pull // amount
    pull = pull * lift // amount
    chance = jax.random.randint(jax.random.fold_in(key, 2), (rows, amount), 0, 4096) + pull
    holders = jax.random.permutation(jax.random.fold_in(key, 3), rows)[jnp.arange(amount) % rows]
    chance = jnp.where(jnp.arange(rows)[:, None] == holders[None, :], 1 << 14, chance)
    priority = chance * amount + jnp.arange(amount)
    return lax.top_k(priority.astype(jnp.int32), top)[1].astype(jnp.int32)


def gaussian(stream_key, extent, spread, limit, pieces=(), kind=jnp.bfloat16):
    level = block_levels(stream_key, extent, pieces, -0.22, 0.18) if pieces else 1.0
    drawn = jax.random.normal(stream_key, extent, jnp.float32) * spread * level
    return jnp.minimum(jnp.maximum(drawn, -limit), limit).astype(kind)


def setup_inputs(seed: int = 0, part: int = 0) -> dict:
    seeds = jax.random.split(jax.random.key(seed), 8)
    part_splits = jax.random.split(jax.random.fold_in(seeds[7], part), 8)
    return {
        "tokens": gaussian(part_splits[0], (TOKENS, D), 1.0, 6.0, ((0, 128),)),
        "cotangent": gaussian(part_splits[1], (TOKENS, D), 1.0, 6.0, ((0, 128),)),
        "expert_ids": different_ones(part_splits[2], TOKENS, EXPERTS, 2, 512),
        "gate_wts": jnp.clip(0.2 + 0.8 * jax.random.uniform(part_splits[3], (TOKENS, 2), jnp.float32) ** block_levels(part_splits[3], (TOKENS, 2), ((0, 128),), -0.2, 0.2), 0.2, 1.0),
        "w_gate": gaussian(seeds[4], (EXPERTS, D, FF), D ** -0.5, 0.09375, ((0, 32), (1, 4))),
        "w_up": gaussian(seeds[5], (EXPERTS, D, FF), D ** -0.5, 0.09375, ((0, 32), (1, 4))),
        "w_down": gaussian(seeds[6], (EXPERTS, FF, D), FF ** -0.5, 0.375, ((0, 32), (1, 4))),
    }


def reference(tokens, cotangent, expert_ids, gate_wts, w_gate, w_up, w_down):
    sources = N_EXPERT * N_TENSOR
    model_width = tokens.shape[1]
    slots_all = EXPERTS * CAP
    flat_ids = expert_ids.reshape(sources, 2 * TOK_DEV)
    onehot = (flat_ids[:, :, None] == jnp.arange(EXPERTS, dtype=jnp.int32)[None, None, :]).astype(jnp.int32)
    positions = jnp.sum(onehot * (jnp.cumsum(onehot, axis=1) - 1), axis=2)
    retained = positions < CAP
    target = jnp.where(retained, flat_ids * CAP + positions, slots_all)

    def invert(row_target):
        return jnp.full((slots_all,), -1, jnp.int32).at[row_target].set(
            jnp.arange(2 * TOK_DEV, dtype=jnp.int32), mode="drop")

    anchor = jax.vmap(invert)(target)
    gate_flat = gate_wts.reshape(sources, 2 * TOK_DEV)
    block_base = (jnp.arange(sources, dtype=jnp.int32) * TOK_DEV)[:, None]
    zero_half = jnp.zeros((), jnp.bfloat16)

    def partial_sum(left, right):
        left_transposed = left.reshape(N_EXPERT, N_TENSOR, CAP, -1).transpose(1, 0, 2, 3)
        left_transposed = left_transposed.reshape(N_TENSOR, N_EXPERT * CAP, -1).astype(jnp.float32)
        right_transposed = right.reshape(N_EXPERT, N_TENSOR, CAP, -1).transpose(1, 0, 2, 3)
        right_transposed = right_transposed.reshape(N_TENSOR, N_EXPERT * CAP, -1).astype(jnp.float32)
        summands = jnp.einsum("aye,aym->aem", left_transposed, right_transposed).astype(jnp.bfloat16)
        summands = lax.optimization_barrier(summands)
        return jnp.sum(summands.astype(jnp.float32), axis=0).astype(jnp.bfloat16)

    def one_expert(expert):
        chosen = lax.dynamic_slice_in_dim(anchor, expert * CAP, CAP, 1)
        populated_rows = (chosen >= 0).reshape(-1)
        picked = jnp.maximum(chosen, 0)
        tok_index = (block_base + picked // 2).reshape(-1)
        rows_in = jnp.where(populated_rows[:, None], tokens[tok_index], zero_half)
        gate_scale = jnp.take_along_axis(gate_flat, picked, axis=1).reshape(-1)
        scaled = (gate_scale[:, None] * cotangent[tok_index].astype(jnp.float32)).astype(jnp.bfloat16)
        cot_in = jnp.where(populated_rows[:, None], scaled, zero_half)
        gate_matrix = w_gate[expert]
        up_mat = w_up[expert]
        down_mat = w_down[expert]
        pre_gate = jnp.dot(rows_in, gate_matrix, preferred_element_type=jnp.float32)
        pre_up = jnp.dot(rows_in, up_mat, preferred_element_type=jnp.float32)
        sigmoid_gate = jax.nn.sigmoid(pre_gate)
        activated = pre_gate * sigmoid_gate
        hidden = (activated * pre_up).astype(jnp.bfloat16)
        grad_hidden = jnp.dot(cot_in, down_mat.T, preferred_element_type=jnp.float32)
        grad_gate_pre = (grad_hidden * pre_up * sigmoid_gate * (1.0 + pre_gate * (1.0 - sigmoid_gate))).astype(jnp.bfloat16)
        grad_up_pre = (grad_hidden * activated).astype(jnp.bfloat16)
        input_rows = (jnp.dot(grad_gate_pre, gate_matrix.T, preferred_element_type=jnp.float32)
                      + jnp.dot(grad_up_pre, up_mat.T, preferred_element_type=jnp.float32)).astype(jnp.bfloat16)
        return (partial_sum(rows_in, grad_gate_pre), partial_sum(rows_in, grad_up_pre),
                partial_sum(hidden, cot_in), input_rows.reshape(sources, CAP, model_width))

    grad_gate, grad_up, grad_down, input_all = lax.map(one_expert, jnp.arange(EXPERTS, dtype=jnp.int32))
    slot_clip = jnp.minimum(positions, CAP - 1).astype(jnp.int32)
    source_index = jnp.broadcast_to(jnp.arange(sources, dtype=jnp.int32)[:, None], flat_ids.shape)
    gathered = input_all[flat_ids, source_index, slot_clip].astype(jnp.float32)
    gathered = jnp.where(retained[:, :, None], gathered, jnp.zeros((), jnp.float32))
    input_grad = jnp.sum(gathered.reshape(sources, TOK_DEV, 2, model_width), axis=2)
    input_grad = input_grad.reshape(TOKENS, model_width).astype(jnp.bfloat16)
    return (input_grad, grad_gate, grad_up, grad_down)
```

```python
import functools

import jax
import jax.numpy as jnp
from jax import lax
from jax.experimental import pallas as pl
from jax.experimental.pallas import tpu as pltpu
from jax.sharding import PartitionSpec as P

BF = jnp.bfloat16
F32 = jnp.float32
MESH = pl.DeviceIdType.MESH


def dot(a, b, ca=1, cb=0):
    return lax.dot_general(a, b, (((ca,), (cb,)), ((), ())), preferred_element_type=F32)


def iota(shape, axis):
    return lax.broadcasted_iota(jnp.int32, shape, axis)


def body(
    sizes,
    ids_ref, gts_ref, tok_hbm, cot_hbm, wg_hbm, wu_hbm, wd_hbm,
    ig_ref, gg_ref, gu_ref, gd_ref,
    tokv, cotv, wg, wu, wd, pick, send, recv, rq, cq, gact, hid, rsend, ret,
    xrow, xact, down, xdown,
    in_sem, ssem, rsem, wssem, wrsem, bssem, brsem, rowss, rowrs, actss, actrs, dss, drs,
):
    E, T, CAP, TOK, D, FF = sizes
    Z = E // 2
    DT = D // T
    FT = FF // T
    ROWS = T * CAP
    GRP = 8
    NG = E // GRP
    GS = GRP * CAP
    SL = E * CAP
    me = lax.axis_index("expert")
    ti = lax.axis_index("tensor")

    def partner(j, sign):
        u = j // 2
        near = (u + 1) // 2
        step = (u % 2) * near + (1 - u % 2) * (Z - near)
        away = step if sign > 0 else Z - step
        return ((me // 2 + away) % Z) * 2 + (me % 2 + j) % 2

    def side(k):
        return (ti + k) % T

    loads = []

    def load(src, dst, k):
        c = pltpu.make_async_copy(src, dst, in_sem.at[k])
        c.start()
        return c

    for q in range(T):
        loads.append(load(tok_hbm.at[:, pl.ds(q * DT, DT)], tokv.at[pl.ds(q * TOK, TOK)], q))
    for q in range(T):
        loads.append(load(cot_hbm.at[:, pl.ds(q * DT, DT)], cotv.at[pl.ds(q * TOK, TOK)], T + q))
    loads.append(load(wg_hbm.at[0], wg.at[ti], 2 * T))
    loads.append(load(wu_hbm.at[0], wu.at[ti], 2 * T + 1))
    loads.append(load(wd_hbm.at[0], wd.at[ti], 2 * T + 2))

    bar = pltpu.get_barrier_semaphore()

    def greet(j, c):
        pl.semaphore_signal(bar, 1, device_id={"expert": partner(j, 1)}, device_id_type=MESH)
        return c

    lax.fori_loop(1, E, greet, 0)
    for k in range(1, T):
        pl.semaphore_signal(bar, 1, device_id={"tensor": side(k)}, device_id_type=MESH)

    W = T * TOK
    i0 = ids_ref[0:1, :]
    i1 = ids_ref[1:2, :]
    ex = iota((E, W), 0)
    h0 = i0 == ex
    h1 = i1 == ex
    both = (jnp.where(h0, 1.0, 0.0) + jnp.where(h1, 1.0, 0.0)).astype(BF)
    ra = iota((W, W), 0)
    rb = iota((W, W), 1)
    before = jnp.where((ra // TOK == rb // TOK) & (ra < rb), 1.0, 0.0).astype(BF)
    count = dot(both, before)
    p0 = jnp.sum(jnp.where(h0, count, 0.0), axis=0, keepdims=True).astype(jnp.int32)
    p1 = jnp.sum(jnp.where(h1, count, 0.0), axis=0, keepdims=True).astype(jnp.int32)
    s0 = jnp.where(p0 < CAP, i0 * CAP + p0, -1)
    s1 = jnp.where(p1 < CAP, i1 * CAP + p1, -1)
    g0 = gts_ref[0:1, :]
    g1 = gts_ref[1:2, :]

    for c in loads[: 2 * T]:
        c.wait()

    EB = 4
    RB = EB * ROWS

    def build(i, c):
        r = iota((RB, W), 0) + i * RB
        slot = (r // ROWS) * CAP + r % CAP
        same = (r // CAP) % T == iota((RB, W), 1) // TOK
        m0 = (s0 == slot) & same
        m1 = (s1 == slot) & same
        o = jnp.where(m0 | m1, 1.0, 0.0).astype(BF)
        gate = jnp.sum(jnp.where(m0, g0, 0.0) + jnp.where(m1, g1, 0.0), axis=1, keepdims=True)
        pick[pl.ds(i * RB, RB), :] = o
        x = dot(o, tokv[...]).astype(BF)
        send[pl.ds(i * EB, EB), 0:ROWS, :] = x.reshape(EB, ROWS, DT)
        y = (gate * dot(o, cotv[...])).astype(BF)
        send[pl.ds(i * EB, EB), ROWS : 2 * ROWS, :] = y.reshape(EB, ROWS, DT)
        return c

    lax.fori_loop(0, E // EB, build, 0)

    pl.semaphore_wait(bar, E - 1 + T - 1)

    def dispatch(j):
        to = partner(j, 1)
        return pltpu.make_async_remote_copy(
            send.at[to], recv.at[j], ssem.at[j], rsem.at[j],
            device_id={"expert": to}, device_id_type=MESH,
        )

    def start_dispatch(j, c):
        dispatch(j).start()
        return c

    lax.fori_loop(1, E, start_dispatch, 0)

    weights = (wg, wu, wd)

    def gather(n, k):
        return pltpu.make_async_remote_copy(
            weights[n].at[ti], weights[n].at[ti], wssem.at[n, k], wrsem.at[n, k],
            device_id={"tensor": side(k)}, device_id_type=MESH,
        )

    def gathered(n, k):
        src = side(T - k)
        return pltpu.make_async_remote_copy(
            weights[n].at[src], weights[n].at[src], wssem.at[n, k], wrsem.at[n, k],
            device_id={"tensor": side(k)}, device_id_type=MESH,
        )

    for n in range(3):
        loads[2 * T + n].wait()
    for n in range(3):
        for k in (1, 3, 2):
            gather(n, k).start()

    recv[0] = send[me]

    MB = 2 * ROWS
    fo = iota((GRP * MB, GRP * MB), 0)
    fi = iota((GRP * MB, GRP * MB), 1)
    want = (((fo % GS) // CAP) * MB) + (fo // (T * GS)) * ROWS + ((fo // GS) % T) * CAP + fo % CAP
    spread = jnp.where(fi == want, 1.0, 0.0).astype(BF)
    bo = iota((GRP * ROWS, GRP * ROWS), 0)
    bi = iota((GRP * ROWS, GRP * ROWS), 1)
    wantb = ((bo // CAP) % T) * GS + (bo // ROWS) * CAP + bo % CAP
    fold = jnp.where(bi == wantb, 1.0, 0.0).astype(BF)

    def wait_dispatch(j, c):
        dispatch(j).wait_recv()
        return c

    def unpack(g):
        lax.fori_loop(max(1, g * GRP), (g + 1) * GRP, wait_dispatch, 0)
        for half in range(2):
            cols = pl.ds(half * (DT // 2), DT // 2)
            m = recv[pl.ds(g * GRP, GRP), :, cols].reshape(GRP * MB, DT // 2)
            v = dot(spread, m).astype(BF)
            for q in range(T):
                rq[q, pl.ds(g * GS, GS), cols] = v[q * GS : (q + 1) * GS]
                cq[q, pl.ds(g * GS, GS), cols] = v[(T + q) * GS : (T + q + 1) * GS]

    def back(j):
        to = partner(j, -1)
        return pltpu.make_async_remote_copy(
            rsend.at[j], ret.at[me], bssem.at[j], brsem.at[me],
            device_id={"expert": to}, device_id_type=MESH,
        )

    def start_back(j, c):
        back(j).start()
        return c

    def expert(lo, hi):
        sl = pl.ds(lo * GS, (hi - lo) * GS)
        pg = sum(dot(rq[q, sl, :], wg[q]) for q in range(T))
        pu = sum(dot(rq[q, sl, :], wu[q]) for q in range(T))
        gh = sum(
            dot(cq[q, sl, :], wd[:, :, q * DT : (q + 1) * DT].reshape(FF, DT), 1, 1)
            for q in range(T)
        )
        sg = jax.nn.sigmoid(pg)
        act = pg * sg
        hid[sl, :] = (act * pu).astype(BF)
        a = (gh * pu * sg * (1.0 + pg * (1.0 - sg))).astype(BF)
        b = (gh * act).astype(BF)
        gact[sl, 0:FF] = a
        gact[sl, FF : 2 * FF] = b
        parts = [(dot(a, wg[q], 1, 1) + dot(b, wu[q], 1, 1)).astype(BF) for q in range(T)]
        for g in range(lo, hi):
            o = (g - lo) * GS
            m = jnp.concatenate([p[o : o + GS] for p in parts], axis=0)
            v = dot(fold, m).astype(BF)
            rsend[pl.ds(g * GRP, GRP)] = v.reshape(GRP, ROWS, DT)
        lax.fori_loop(max(1, lo * GRP), hi * GRP, start_back, 0)

    def rows_to(h, k):
        lo, n = (0, (NG - 1) * GS) if h == 0 else ((NG - 1) * GS, GS)
        return pltpu.make_async_remote_copy(
            rq.at[side(k), pl.ds(lo, n)], xrow.at[ti, pl.ds(lo, n)], rowss.at[h, k], rowrs.at[h, k],
            device_id={"tensor": side(k)}, device_id_type=MESH,
        )

    def act_to(k):
        return pltpu.make_async_remote_copy(
            gact, xact.at[ti], actss.at[k], actrs.at[k],
            device_id={"tensor": side(k)}, device_id_type=MESH,
        )

    def down_to(k):
        return pltpu.make_async_remote_copy(
            down.at[side(k)], xdown.at[ti], dss.at[k], drs.at[k],
            device_id={"tensor": side(k)}, device_id_type=MESH,
        )

    for g in range(NG - 1):
        unpack(g)
    for k in (1, 3, 2):
        rows_to(0, k).start()
    for n in range(3):
        for k in range(1, T):
            gathered(n, k).wait_recv()
    expert(0, NG - 1)
    unpack(NG - 1)
    expert(NG - 1, NG)
    for k in (1, 3, 2):
        rows_to(1, k).start()
        act_to(k).start()

    ht = hid[...].astype(F32).T.astype(BF)
    for q in range(T):
        v = dot(ht, cq[q]).astype(BF)
        for t in range(T):
            down[t, :, q * DT : (q + 1) * DT] = v[t * FT : (t + 1) * FT]
    for k in (1, 3, 2):
        down_to(k).start()

    xrow[ti] = rq[ti]
    xact[ti] = gact[...]
    ret[me] = rsend[0]
    xdown[ti] = down[ti]
    for k in range(1, T):
        rows_to(0, k).wait_recv()
        rows_to(1, k).wait_recv()
        act_to(k).wait_recv()
    acts = xact[...].reshape(T * SL, 2 * FF)
    CB = 256
    for n in range(DT // CB):
        r = xrow[:, :, n * CB : (n + 1) * CB].reshape(T * SL, CB)
        v = dot(r, acts, 0, 0).astype(BF)
        gg_ref[0, n * CB : (n + 1) * CB, :] = v[:, 0:FF]
        gu_ref[0, n * CB : (n + 1) * CB, :] = v[:, FF : 2 * FF]

    for k in range(1, T):
        down_to(k).wait_recv()
    for n in range(T):
        cols = pl.ds(n * DT, DT)
        v = xdown[0, :, cols].astype(F32)
        for t in range(1, T):
            v = v + xdown[t, :, cols].astype(F32)
        gd_ref[0, :, cols] = v.astype(BF)

    unpick = pick[...].astype(F32).T.astype(BF)

    def wait_back(j, c):
        src = partner(j, 1)
        pltpu.make_async_remote_copy(
            rsend.at[j], ret.at[src], bssem.at[j], brsem.at[src],
            device_id={"expert": src}, device_id_type=MESH,
        ).wait_recv()
        return c

    lax.fori_loop(1, E, wait_back, 0)
    for n in range(DT // CB):
        r = ret[:, :, n * CB : (n + 1) * CB].reshape(E * ROWS, CB)
        v = dot(unpick, r).astype(BF)
        for q in range(T):
            ig_ref[:, q * DT + n * CB : q * DT + (n + 1) * CB] = v[q * TOK : (q + 1) * TOK]

    def drain(j, c):
        dispatch(j).wait_send()
        back(j).wait_send()
        return c

    lax.fori_loop(1, E, drain, 0)
    for k in range(1, T):
        for n in range(3):
            gather(n, k).wait_send()
        rows_to(0, k).wait_send()
        rows_to(1, k).wait_send()
        act_to(k).wait_send()
        down_to(k).wait_send()


def local(tokens, cotangent, expert_ids, gate_wts, w_gate, w_up, w_down):
    TOK, D = tokens.shape
    E = lax.axis_size("expert")
    T = lax.axis_size("tensor")
    FF = w_gate.shape[2]
    CAP = 2 * TOK // E
    DT, FT, SL, ROWS = D // T, FF // T, E * CAP, T * CAP
    ids = jnp.tile(expert_ids.T, (1, T))
    gts = jnp.tile(gate_wts.T, (1, T))
    vm = pl.BlockSpec(memory_space=pltpu.VMEM)
    hb = pl.BlockSpec(memory_space=pl.ANY)
    dma = pltpu.SemaphoreType.DMA
    return pl.pallas_call(
        functools.partial(body, (E, T, CAP, TOK, D, FF)),
        name="routed_backward",
        out_shape=(
            jax.ShapeDtypeStruct((TOK, D), BF),
            jax.ShapeDtypeStruct((1, DT, FF), BF),
            jax.ShapeDtypeStruct((1, DT, FF), BF),
            jax.ShapeDtypeStruct((1, FT, D), BF),
        ),
        in_specs=[vm, vm, hb, hb, hb, hb, hb],
        out_specs=(vm, vm, vm, vm),
        scratch_shapes=[
            pltpu.VMEM((T * TOK, DT), BF),
            pltpu.VMEM((T * TOK, DT), BF),
            pltpu.VMEM((T, DT, FF), BF),
            pltpu.VMEM((T, DT, FF), BF),
            pltpu.VMEM((T, FT, D), BF),
            pltpu.VMEM((E * ROWS, T * TOK), BF),
            pltpu.VMEM((E, 2 * ROWS, DT), BF),
            pltpu.VMEM((E, 2 * ROWS, DT), BF),
            pltpu.VMEM((T, SL, DT), BF),
            pltpu.VMEM((T, SL, DT), BF),
            pltpu.VMEM((SL, 2 * FF), BF),
            pltpu.VMEM((SL, FF), BF),
            pltpu.VMEM((E, ROWS, DT), BF),
            pltpu.VMEM((E, ROWS, DT), BF),
            pltpu.VMEM((T, SL, DT), BF),
            pltpu.VMEM((T, SL, 2 * FF), BF),
            pltpu.VMEM((T, FT, D), BF),
            pltpu.VMEM((T, FT, D), BF),
            dma((2 * T + 3,)),
            dma((E,)), dma((E,)),
            dma((3, T)), dma((3, T)),
            dma((E,)), dma((E,)),
            dma((2, T)), dma((2, T)),
            dma((T,)), dma((T,)),
            dma((T,)), dma((T,)),
        ],
        compiler_params=pltpu.CompilerParams(
            collective_id=0, has_side_effects=True, vmem_limit_bytes=56 << 20
        ),
    )(ids, gts, tokens, cotangent, w_gate, w_up, w_down)


def solution(mesh):
    rows = P(("group", "expert", "tensor"), None)
    grads = P(("group", "expert"), "tensor", None)
    return jax.shard_map(
        local,
        mesh=mesh,
        in_specs=(rows, rows, rows, rows) + (P("expert", "tensor", None),) * 3,
        out_specs=(rows, grads, grads, grads),
        check_vma=False,
    )
```

```python
import functools

import jax
import jax.numpy as jnp
from jax import lax
from jax.experimental import pallas as pl
from jax.experimental.pallas import tpu as pltpu
from jax.sharding import PartitionSpec as P

BF = jnp.bfloat16
F32 = jnp.float32
MESH = pl.DeviceIdType.MESH


def dot(a, b, ca=1, cb=0):
    return lax.dot_general(a, b, (((ca,), (cb,)), ((), ())), preferred_element_type=F32)


def iota(shape, axis):
    return lax.broadcasted_iota(jnp.int32, shape, axis)


def body(
    sizes,
    ids_hbm, gts_hbm, tok_hbm, cot_hbm, wg_hbm, wu_hbm, wd_hbm,
    ig_ref, gg_ref, gu_ref, gd_ref,
    idv, gtv, tokv, cotv, wg, wu, wd, pick, send, recv, rc, gact, rsend, ret, xrc, xact, down,
    from_up, from_below, in_sem, ssem, rsem, wssem, wrsem, bssem, brsem, rcss, rcrs, actss, actrs, dss, drs,
):
    E, T, CAP, TOK, D, FF = sizes
    Z = E // 2
    DT = D // T
    FT = FF // T
    ROWS = T * CAP
    GRP = 8
    NG = E // GRP
    GS = GRP * CAP
    SL = E * CAP
    me = lax.axis_index("expert")
    ti = lax.axis_index("tensor")

    def partner(j, sign):
        u = j // 2
        near = (u + 1) // 2
        step = (u % 2) * near + (1 - u % 2) * (Z - near)
        away = step if sign > 0 else Z - step
        return ((me // 2 + away) % Z) * 2 + (me % 2 + j) % 2

    def side(k):
        return (ti + k) % T

    bar = pltpu.get_barrier_semaphore()
    z, core = me // 2, me % 2
    up, below = (z + 1) % Z, (z + Z - 1) % Z
    near_by = [z * 2 + 1 - core, up * 2 + core, up * 2 + 1 - core, below * 2 + core, below * 2 + 1 - core]
    for e in near_by:
        pl.semaphore_signal(bar, 1, device_id={"expert": e}, device_id_type=MESH)
    for k in range(1, T):
        pl.semaphore_signal(bar, 1, device_id={"tensor": side(k)}, device_id_type=MESH)

    def tell_up(k):
        pl.semaphore_signal(from_below.at[k], 1, device_id={"expert": up * 2 + core}, device_id_type=MESH)

    def tell_below(k):
        pl.semaphore_signal(from_up.at[k], 1, device_id={"expert": below * 2 + core}, device_id_type=MESH)

    loads = []

    def load(src, dst, k):
        c = pltpu.make_async_copy(src, dst, in_sem.at[k])
        c.start()
        return c

    head = [load(ids_hbm, idv, 2 * T + 3), load(gts_hbm, gtv, 2 * T + 4)]
    for q in range(T):
        loads.append(load(tok_hbm.at[:, pl.ds(q * DT, DT)], tokv.at[pl.ds(q * TOK, TOK)], q))
    for q in range(T):
        loads.append(load(cot_hbm.at[:, pl.ds(q * DT, DT)], cotv.at[pl.ds(q * TOK, TOK)], T + q))
    loads.append(load(wg_hbm.at[0], wg.at[ti], 2 * T))
    loads.append(load(wu_hbm.at[0], wu.at[ti], 2 * T + 1))
    loads.append(load(wd_hbm.at[0], wd.at[ti], 2 * T + 2))

    W = T * TOK
    for c in head:
        c.wait()
    ids = jnp.concatenate([idv[...]] * T, axis=1)
    gts = jnp.concatenate([gtv[...]] * T, axis=1)
    i0 = ids[0:1, :]
    i1 = ids[1:2, :]
    ex = iota((E, W), 0)
    h0 = i0 == ex
    h1 = i1 == ex
    both = (jnp.where(h0, 1.0, 0.0) + jnp.where(h1, 1.0, 0.0)).astype(BF)
    ra = iota((W, W), 0)
    rb = iota((W, W), 1)
    before = jnp.where((ra // TOK == rb // TOK) & (ra < rb), 1.0, 0.0).astype(BF)
    count = dot(both, before)
    p0 = jnp.sum(jnp.where(h0, count, 0.0), axis=0, keepdims=True).astype(jnp.int32)
    p1 = jnp.sum(jnp.where(h1, count, 0.0), axis=0, keepdims=True).astype(jnp.int32)
    s0 = jnp.where(p0 < CAP, i0 * CAP + p0, -1)
    s1 = jnp.where(p1 < CAP, i1 * CAP + p1, -1)
    g0 = gts[0:1, :]
    g1 = gts[1:2, :]

    for c in loads[: 2 * T]:
        c.wait()

    EB = 4
    RB = EB * ROWS

    def dispatch(j):
        return pltpu.make_async_remote_copy(
            send.at[j], recv.at[j], ssem.at[j], rsem.at[j],
            device_id={"expert": partner(j, 1)}, device_id_type=MESH,
        )

    def build(i):
        r = iota((RB, 1), 0) + i * RB
        j = r // ROWS
        u = j // 2
        near = (u + 1) // 2
        step = jnp.where(u % 2 == 1, near, Z - near)
        slot = (((z + step) % Z) * 2 + (core + j) % 2) * CAP + r % CAP
        same = (r // CAP) % T == iota((1, W), 1) // TOK
        m0 = (s0 == slot) & same
        m1 = (s1 == slot) & same
        o = jnp.where(m0 | m1, 1.0, 0.0).astype(BF)
        gate = jnp.sum(jnp.where(m0, g0, 0.0) + jnp.where(m1, g1, 0.0), axis=1, keepdims=True)
        pick[pl.ds(i * RB, RB), :] = o
        x = dot(o, tokv[...]).astype(BF)
        send[pl.ds(i * EB, EB), 0:ROWS, :] = x.reshape(EB, ROWS, DT)
        y = (gate * dot(o, cotv[...])).astype(BF)
        send[pl.ds(i * EB, EB), ROWS : 2 * ROWS, :] = y.reshape(EB, ROWS, DT)

    weights = (wg, wu, wd)

    def gather(n, k):
        return pltpu.make_async_remote_copy(
            weights[n].at[ti], weights[n].at[ti], wssem.at[n, k], wrsem.at[n, k],
            device_id={"tensor": side(1 if k == 0 else T - 1)}, device_id_type=MESH,
        )

    def gathered(n, k):
        src = side(T - 1 if k == 0 else 1)
        return pltpu.make_async_remote_copy(
            weights[n].at[src], weights[n].at[src], wssem.at[n, k], wrsem.at[n, k],
            device_id={"tensor": side(1)}, device_id_type=MESH,
        )

    def pass_on(n, k):
        h = weights[n].shape[1] // 2
        part = weights[n].at[side(T - 1 if k == 0 else 1), pl.ds(k * h, h)]
        return pltpu.make_async_remote_copy(
            part, part, wssem.at[n, 2 + k], wrsem.at[n, 2 + k],
            device_id={"tensor": side(1 if k == 0 else T - 1)}, device_id_type=MESH,
        )

    def passed_on(n, k):
        h = weights[n].shape[1] // 2
        part = weights[n].at[side(2), pl.ds(k * h, h)]
        return pltpu.make_async_remote_copy(
            part, part, wssem.at[n, 2 + k], wrsem.at[n, 2 + k],
            device_id={"tensor": side(1)}, device_id_type=MESH,
        )

    build(0)
    pl.semaphore_wait(bar, len(near_by) + T - 1)
    tell_below(1)
    tell_up(1)
    for j in range(1, EB):
        dispatch(j).start()
    for n in range(3):
        loads[2 * T + n].wait()
    for n in range(3):
        for k in range(2):
            gather(n, k).start()
    NC = E // EB

    def chunk(i, c):
        build(i)
        pl.semaphore_wait(from_up.at[i], 1)

        @pl.when(i < NC - 1)
        def _():
            tell_below(i + 1)

        @pl.when(i > 1)
        def _():
            pl.semaphore_wait(from_below.at[i - 1], 1)

            @pl.when(i < NC - 1)
            def _():
                tell_up(i)

        for j in range(EB):
            dispatch(i * EB + j).start()
        return c

    lax.fori_loop(1, NC, chunk, 0)
    recv[0] = send[0]

    MB = 2 * ROWS
    fo = iota((GRP * MB, GRP * MB), 0)
    fi = iota((GRP * MB, GRP * MB), 1)
    want = (((fo % GS) // CAP) * MB) + (fo // (T * GS)) * ROWS + ((fo // GS) % T) * CAP + fo % CAP
    spread = jnp.where(fi == want, 1.0, 0.0).astype(BF)
    bo = iota((GRP * ROWS, GRP * ROWS), 0)
    bi = iota((GRP * ROWS, GRP * ROWS), 1)
    wantb = ((bo // CAP) % T) * GS + (bo // ROWS) * CAP + bo % CAP
    fold = jnp.where(bi == wantb, 1.0, 0.0).astype(BF)

    def wait_dispatch(j, c):
        dispatch(j).wait_recv()
        return c

    def unpack(g):
        lax.fori_loop(max(1, g * GRP), (g + 1) * GRP, wait_dispatch, 0)
        for half in range(2):
            cols = pl.ds(half * (DT // 2), DT // 2)
            m = recv[pl.ds(g * GRP, GRP), :, cols].reshape(GRP * MB, DT // 2)
            v = dot(spread, m).astype(BF)
            for q in range(T):
                rc[q, pl.ds(g * GS, GS), cols] = v[q * GS : (q + 1) * GS]
                cols2 = pl.ds(DT + half * (DT // 2), DT // 2)
                rc[q, pl.ds(g * GS, GS), cols2] = v[(T + q) * GS : (T + q + 1) * GS]

    def back(j):
        to = partner(j, -1)
        return pltpu.make_async_remote_copy(
            rsend.at[j], ret.at[j], bssem.at[j], brsem.at[j],
            device_id={"expert": to}, device_id_type=MESH,
        )

    def start_back(j, c):
        back(j).start()
        return c

    def expert(lo, hi):
        sl = pl.ds(lo * GS, (hi - lo) * GS)
        pg = sum(dot(rc[q, sl, 0:DT], wg[q]) for q in range(T))
        pu = sum(dot(rc[q, sl, 0:DT], wu[q]) for q in range(T))
        gh = sum(
            dot(rc[q, sl, DT : 2 * DT], wd[:, :, q * DT : (q + 1) * DT].reshape(FF, DT), 1, 1)
            for q in range(T)
        )
        sg = jax.nn.sigmoid(pg)
        act = pg * sg
        gact[sl, 2 * FF : 3 * FF] = (act * pu).astype(BF)
        a = (gh * pu * sg * (1.0 + pg * (1.0 - sg))).astype(BF)
        b = (gh * act).astype(BF)
        gact[sl, 0:FF] = a
        gact[sl, FF : 2 * FF] = b
        parts = [(dot(a, wg[q], 1, 1) + dot(b, wu[q], 1, 1)).astype(BF) for q in range(T)]
        for g in range(lo, hi):
            o = (g - lo) * GS
            m = jnp.concatenate([p[o : o + GS] for p in parts], axis=0)
            v = dot(fold, m).astype(BF)
            rsend[pl.ds(g * GRP, GRP)] = v.reshape(GRP, ROWS, DT)
        lax.fori_loop(max(1, lo * GRP), hi * GRP, start_back, 0)

    def part_of(h):
        return pl.ds(0, (NG - 1) * GS) if h == 0 else pl.ds((NG - 1) * GS, GS)

    def rows_to(h, k):
        return pltpu.make_async_remote_copy(
            rc.at[side(k), part_of(h)], xrc.at[ti, part_of(h)], rcss.at[h, k], rcrs.at[h, k],
            device_id={"tensor": side(k)}, device_id_type=MESH,
        )

    def act_to(h, k):
        return pltpu.make_async_remote_copy(
            gact.at[part_of(h)], xact.at[ti, part_of(h)], actss.at[h, k], actrs.at[h, k],
            device_id={"tensor": side(k)}, device_id_type=MESH,
        )

    mine = pl.ds(pl.multiple_of(ti * DT, DT), DT)

    def down_to(k):
        return pltpu.make_async_remote_copy(
            down.at[side(k)], gd_ref.at[0, :, mine], dss.at[k], drs.at[k],
            device_id={"tensor": side(k)}, device_id_type=MESH,
        )

    unpack(0)
    unpack(1)
    for n in range(3):
        for k in range(2):
            gathered(n, k).wait_recv()
            pass_on(n, k).start()
    for g in range(2, NG - 1):
        unpack(g)
    for k in (1, 3, 2):
        rows_to(0, k).start()
    for n in range(3):
        for k in range(2):
            passed_on(n, k).wait_recv()
    expert(0, NG - 1)
    for k in (1, 3, 2):
        act_to(0, k).start()
    unpack(NG - 1)
    for k in (1, 3, 2):
        rows_to(1, k).start()
    expert(NG - 1, NG)
    for k in (1, 3, 2):
        act_to(1, k).start()
    xrc[ti] = rc[ti]
    xact[ti] = gact[...]
    ret[0] = rsend[0]
    for h in range(2):
        for k in range(1, T):
            rows_to(h, k).wait_recv()
            act_to(h, k).wait_recv()
    CB = 256
    acts = xact[:, :, 2 * FF : 3 * FF].reshape(T * SL, FF)
    for n in range(DT // CB):
        r = xrc[:, :, DT + n * CB : DT + (n + 1) * CB].reshape(T * SL, CB)
        v = dot(acts, r, 0, 0).astype(BF)
        down[:, :, n * CB : (n + 1) * CB] = v.reshape(T, FT, CB)
    for k in (1, 3, 2):
        down_to(k).start()
    gd_ref[0, :, mine] = down[ti]
    acts = xact[:, :, 0 : 2 * FF].reshape(T * SL, 2 * FF)
    for n in range(DT // CB):
        r = xrc[:, :, n * CB : (n + 1) * CB].reshape(T * SL, CB)
        v = dot(r, acts, 0, 0).astype(BF)
        gg_ref[0, n * CB : (n + 1) * CB, :] = v[:, 0:FF]
        gu_ref[0, n * CB : (n + 1) * CB, :] = v[:, FF : 2 * FF]

    unpick = pick[...].astype(F32).T.astype(BF)

    def wait_back(j, c):
        back(j).wait_recv()
        return c

    lax.fori_loop(1, E, wait_back, 0)
    for n in range(DT // CB):
        r = ret[:, :, n * CB : (n + 1) * CB].reshape(E * ROWS, CB)
        v = dot(unpick, r).astype(BF)
        for q in range(T):
            ig_ref[:, q * DT + n * CB : q * DT + (n + 1) * CB] = v[q * TOK : (q + 1) * TOK]

    def drain(j, c):
        dispatch(j).wait_send()
        back(j).wait_send()
        return c

    lax.fori_loop(1, E, drain, 0)
    for n in range(3):
        for k in range(2):
            gather(n, k).wait_send()
            pass_on(n, k).wait_send()
    for k in range(1, T):
        for h in range(2):
            rows_to(h, k).wait_send()
            act_to(h, k).wait_send()
        down_to(k).wait_send()
        down_to(k).wait_recv()


def put(*refs):
    n = (len(refs) - 1) // 2
    copies = [pltpu.make_async_copy(refs[i], refs[n + i], refs[-1].at[i]) for i in range(n)]
    for c in copies:
        c.start()
    for c in copies:
        c.wait()


def local(tokens, cotangent, expert_ids, gate_wts, w_gate, w_up, w_down):
    TOK, D = tokens.shape
    E = lax.axis_size("expert")
    T = lax.axis_size("tensor")
    FF = w_gate.shape[2]
    CAP = 2 * TOK // E
    DT, FT, SL, ROWS = D // T, FF // T, E * CAP, T * CAP
    shapes = ((TOK, D), (1, DT, FF), (1, DT, FF), (1, FT, D))
    vm = pl.BlockSpec(memory_space=pltpu.VMEM)
    hb = pl.BlockSpec(memory_space=pl.ANY)
    dma = pltpu.SemaphoreType.DMA
    outs = pl.pallas_call(
        functools.partial(body, (E, T, CAP, TOK, D, FF)),
        name="routed_backward",
        out_shape=tuple(pltpu.VMEM(s, BF) for s in shapes),
        in_specs=[hb] * 7,
        out_specs=(vm, vm, vm, vm),
        scratch_shapes=[
            pltpu.VMEM((2, TOK), jnp.int32),
            pltpu.VMEM((2, TOK), F32),
            pltpu.VMEM((T * TOK, DT), BF),
            pltpu.VMEM((T * TOK, DT), BF),
            pltpu.VMEM((T, DT, FF), BF),
            pltpu.VMEM((T, DT, FF), BF),
            pltpu.VMEM((T, FT, D), BF),
            pltpu.VMEM((E * ROWS, T * TOK), BF),
            pltpu.VMEM((E, 2 * ROWS, DT), BF),
            pltpu.VMEM((E, 2 * ROWS, DT), BF),
            pltpu.VMEM((T, SL, 2 * DT), BF),
            pltpu.VMEM((SL, 3 * FF), BF),
            pltpu.VMEM((E, ROWS, DT), BF),
            pltpu.VMEM((E, ROWS, DT), BF),
            pltpu.VMEM((T, SL, 2 * DT), BF),
            pltpu.VMEM((T, SL, 3 * FF), BF),
            pltpu.VMEM((T, FT, DT), BF),
            pltpu.SemaphoreType.REGULAR((E // 4,)), pltpu.SemaphoreType.REGULAR((E // 4,)),
            dma((2 * T + 5,)),
            dma((E,)), dma((E,)),
            dma((3, 4)), dma((3, 4)),
            dma((E,)), dma((E,)),
            dma((2, T)), dma((2, T)),
            dma((2, T)), dma((2, T)),
            dma((T,)), dma((T,)),
        ],
        compiler_params=pltpu.CompilerParams(
            collective_id=0, has_side_effects=True, vmem_limit_bytes=56 << 20
        ),
    )(expert_ids.T, gate_wts.T, tokens, cotangent, w_gate, w_up, w_down)
    outs = [pltpu.with_memory_space_constraint(o, pltpu.VMEM) for o in outs]
    return pl.pallas_call(
        put,
        name="put",
        out_shape=tuple(jax.ShapeDtypeStruct(s, BF) for s in shapes),
        in_specs=[vm] * 4,
        out_specs=(hb,) * 4,
        scratch_shapes=[dma((4,))],
    )(*outs)


def solution(mesh):
    rows = P(("group", "expert", "tensor"), None)
    grads = P(("group", "expert"), "tensor", None)
    return jax.shard_map(
        local,
        mesh=mesh,
        in_specs=(rows, rows, rows, rows) + (P("expert", "tensor", None),) * 3,
        out_specs=(rows, grads, grads, grads),
        check_vma=False,
    )
```

```python
import functools

import jax
import jax.numpy as jnp
from jax import lax
from jax.experimental import pallas as pl
from jax.experimental.pallas import tpu as pltpu
from jax.sharding import PartitionSpec as P

BF = jnp.bfloat16
F32 = jnp.float32
MESH = pl.DeviceIdType.MESH


def dot(a, b, ca=1, cb=0):
    return lax.dot_general(a, b, (((ca,), (cb,)), ((), ())), preferred_element_type=F32)


def iota(shape, axis):
    return lax.broadcasted_iota(jnp.int32, shape, axis)


def body(
    sizes,
    ids_hbm, gts_hbm, tok_hbm, cot_hbm, wg_hbm, wu_hbm, wd_hbm,
    ig_ref, gg_ref, gu_ref, gd_ref,
    idv, gtv, tokv, cotv, wg, wu, wd, pick, send, recv, rc, gact, rsend, ret, xrc, xact, down,
    from_up, from_below, in_sem, ssem, rsem, wssem, wrsem, bssem, brsem, rcss, rcrs, actss, actrs, dss, drs,
):
    E, T, CAP, TOK, D, FF = sizes
    Z = E // 2
    DT = D // T
    FT = FF // T
    ROWS = T * CAP
    GRP = 8
    NG = E // GRP
    GS = GRP * CAP
    SL = E * CAP
    me = lax.axis_index("expert")
    ti = lax.axis_index("tensor")

    def partner(j, sign):
        u = j // 2
        near = (u + 1) // 2
        step = (u % 2) * near + (1 - u % 2) * (Z - near)
        away = step if sign > 0 else Z - step
        return ((me // 2 + away) % Z) * 2 + (me % 2 + j) % 2

    def side(k):
        return (ti + k) % T

    bar = pltpu.get_barrier_semaphore()
    z, core = me // 2, me % 2
    up, below = (z + 1) % Z, (z + Z - 1) % Z
    near_by = [z * 2 + 1 - core, up * 2 + core, up * 2 + 1 - core, below * 2 + core, below * 2 + 1 - core]
    for e in near_by:
        pl.semaphore_signal(bar, 1, device_id={"expert": e}, device_id_type=MESH)
    for k in (1, T - 1):
        pl.semaphore_signal(bar, 1, device_id={"tensor": side(k)}, device_id_type=MESH)

    def tell_up(k):
        pl.semaphore_signal(from_below.at[k], 1, device_id={"expert": up * 2 + core}, device_id_type=MESH)

    def tell_below(k):
        pl.semaphore_signal(from_up.at[k], 1, device_id={"expert": below * 2 + core}, device_id_type=MESH)

    loads = []

    def load(src, dst, k):
        c = pltpu.make_async_copy(src, dst, in_sem.at[k])
        c.start()
        return c

    head = [load(ids_hbm, idv, 2 * T + 3), load(gts_hbm, gtv, 2 * T + 4)]
    for q in range(T):
        loads.append(load(tok_hbm.at[:, pl.ds(q * DT, DT)], tokv.at[pl.ds(q * TOK, TOK)], q))
    for q in range(T):
        loads.append(load(cot_hbm.at[:, pl.ds(q * DT, DT)], cotv.at[pl.ds(q * TOK, TOK)], T + q))
    loads.append(load(wg_hbm.at[0], wg.at[ti], 2 * T))
    loads.append(load(wu_hbm.at[0], wu.at[ti], 2 * T + 1))
    loads.append(load(wd_hbm.at[0], wd.at[ti], 2 * T + 2))

    W = T * TOK
    for c in head:
        c.wait()
    i0 = idv[0:1, :]
    i1 = idv[1:2, :]
    ex = iota((E, TOK), 0)
    h0 = i0 == ex
    h1 = i1 == ex
    both = (jnp.where(h0, 1.0, 0.0) + jnp.where(h1, 1.0, 0.0)).astype(BF)
    before = jnp.where(iota((TOK, TOK), 0) < iota((TOK, TOK), 1), 1.0, 0.0).astype(BF)
    count = dot(both, before)
    p0 = jnp.sum(jnp.where(h0, count, 0.0), axis=0, keepdims=True).astype(jnp.int32)
    p1 = jnp.sum(jnp.where(h1, count, 0.0), axis=0, keepdims=True).astype(jnp.int32)

    def wide(v):
        return jnp.concatenate([v] * T, axis=1)

    s0 = wide(jnp.where(p0 < CAP, i0 * CAP + p0, -1))
    s1 = wide(jnp.where(p1 < CAP, i1 * CAP + p1, -1))
    g0 = wide(gtv[0:1, :])
    g1 = wide(gtv[1:2, :])

    for c in loads[: 2 * T]:
        c.wait()

    EB = 4
    RB = EB * ROWS

    def dispatch(j):
        return pltpu.make_async_remote_copy(
            send.at[j], recv.at[j], ssem.at[j], rsem.at[j],
            device_id={"expert": partner(j, 1)}, device_id_type=MESH,
        )

    def build(i):
        r = iota((RB, 1), 0) + i * RB
        j = r // ROWS
        u = j // 2
        near = (u + 1) // 2
        step = jnp.where(u % 2 == 1, near, Z - near)
        slot = (((z + step) % Z) * 2 + (core + j) % 2) * CAP + r % CAP
        same = (r // CAP) % T == iota((1, W), 1) // TOK
        m0 = (s0 == slot) & same
        m1 = (s1 == slot) & same
        o = jnp.where(m0 | m1, 1.0, 0.0).astype(BF)
        gate = jnp.sum(jnp.where(m0, g0, 0.0) + jnp.where(m1, g1, 0.0), axis=1, keepdims=True)
        pick[pl.ds(i * RB, RB), :] = o
        x = dot(o, tokv[...]).astype(BF)
        send[pl.ds(i * EB, EB), 0:ROWS, :] = x.reshape(EB, ROWS, DT)
        y = (gate * dot(o, cotv[...])).astype(BF)
        send[pl.ds(i * EB, EB), ROWS : 2 * ROWS, :] = y.reshape(EB, ROWS, DT)

    weights = (wg, wu, wd)

    def gather(n, k):
        return pltpu.make_async_remote_copy(
            weights[n].at[ti], weights[n].at[ti], wssem.at[n, k], wrsem.at[n, k],
            device_id={"tensor": side(1 if k == 0 else T - 1)}, device_id_type=MESH,
        )

    def gathered(n, k):
        src = side(T - 1 if k == 0 else 1)
        return pltpu.make_async_remote_copy(
            weights[n].at[src], weights[n].at[src], wssem.at[n, k], wrsem.at[n, k],
            device_id={"tensor": side(1)}, device_id_type=MESH,
        )

    def pass_on(n, k):
        h = weights[n].shape[1] // 2
        part = weights[n].at[side(T - 1 if k == 0 else 1), pl.ds(k * h, h)]
        return pltpu.make_async_remote_copy(
            part, part, wssem.at[n, 2 + k], wrsem.at[n, 2 + k],
            device_id={"tensor": side(1 if k == 0 else T - 1)}, device_id_type=MESH,
        )

    def passed_on(n, k):
        h = weights[n].shape[1] // 2
        part = weights[n].at[side(2), pl.ds(k * h, h)]
        return pltpu.make_async_remote_copy(
            part, part, wssem.at[n, 2 + k], wrsem.at[n, 2 + k],
            device_id={"tensor": side(1)}, device_id_type=MESH,
        )

    build(0)
    pl.semaphore_wait(bar, len(near_by) + 2)
    tell_below(1)
    tell_up(1)
    for j in range(1, EB):
        dispatch(j).start()
    for n in range(3):
        loads[2 * T + n].wait()
    for n in range(3):
        for k in range(2):
            gather(n, k).start()
    NC = E // EB

    def chunk(i, c):
        build(i)
        pl.semaphore_wait(from_up.at[i], 1)

        @pl.when(i < NC - 1)
        def _():
            tell_below(i + 1)

        @pl.when(i > 1)
        def _():
            pl.semaphore_wait(from_below.at[i - 1], 1)

            @pl.when(i < NC - 1)
            def _():
                tell_up(i)

        for j in range(EB):
            dispatch(i * EB + j).start()
        return c

    lax.fori_loop(1, NC, chunk, 0)
    recv[0] = send[0]

    MB = 2 * ROWS
    fo = iota((GRP * MB, GRP * MB), 0)
    fi = iota((GRP * MB, GRP * MB), 1)
    want = (((fo % GS) // CAP) * MB) + (fo // (T * GS)) * ROWS + ((fo // GS) % T) * CAP + fo % CAP
    spread = jnp.where(fi == want, 1.0, 0.0).astype(BF)
    bo = iota((GRP * ROWS, GRP * ROWS), 0)
    bi = iota((GRP * ROWS, GRP * ROWS), 1)
    wantb = ((bo // CAP) % T) * GS + (bo // ROWS) * CAP + bo % CAP
    fold = jnp.where(bi == wantb, 1.0, 0.0).astype(BF)

    def wait_dispatch(j, c):
        dispatch(j).wait_recv()
        return c

    def unpack(g):
        lax.fori_loop(max(1, g * GRP), (g + 1) * GRP, wait_dispatch, 0)
        for half in range(2):
            cols = pl.ds(half * (DT // 2), DT // 2)
            m = recv[pl.ds(g * GRP, GRP), :, cols].reshape(GRP * MB, DT // 2)
            v = dot(spread, m).astype(BF)
            for q in range(T):
                rc[q, pl.ds(g * GS, GS), cols] = v[q * GS : (q + 1) * GS]
                cols2 = pl.ds(DT + half * (DT // 2), DT // 2)
                rc[q, pl.ds(g * GS, GS), cols2] = v[(T + q) * GS : (T + q + 1) * GS]

    def back(j):
        to = partner(j, -1)
        return pltpu.make_async_remote_copy(
            rsend.at[j], ret.at[j], bssem.at[j], brsem.at[j],
            device_id={"expert": to}, device_id_type=MESH,
        )

    def start_back(j, last):
        back(last - j).start()
        return last

    def expert(lo, hi):
        sl = pl.ds(lo * GS, (hi - lo) * GS)
        pg = sum(dot(rc[q, sl, 0:DT], wg[q]) for q in range(T))
        pu = sum(dot(rc[q, sl, 0:DT], wu[q]) for q in range(T))
        gh = sum(
            dot(rc[q, sl, DT : 2 * DT], wd[:, :, q * DT : (q + 1) * DT].reshape(FF, DT), 1, 1)
            for q in range(T)
        )
        sg = jax.nn.sigmoid(pg)
        act = pg * sg
        gact[sl, 2 * FF : 3 * FF] = (act * pu).astype(BF)
        a = (gh * pu * sg * (1.0 + pg * (1.0 - sg))).astype(BF)
        b = (gh * act).astype(BF)
        gact[sl, 0:FF] = a
        gact[sl, FF : 2 * FF] = b
        parts = [(dot(a, wg[q], 1, 1) + dot(b, wu[q], 1, 1)).astype(BF) for q in range(T)]
        for g in range(lo, hi):
            o = (g - lo) * GS
            m = jnp.concatenate([p[o : o + GS] for p in parts], axis=0)
            v = dot(fold, m).astype(BF)
            rsend[pl.ds(g * GRP, GRP)] = v.reshape(GRP, ROWS, DT)
        lax.fori_loop(max(1, lo * GRP), hi * GRP, start_back, max(1, lo * GRP) + hi * GRP - 1)

    def part_of(h):
        return pl.ds(0, (NG - 1) * GS) if h == 0 else pl.ds((NG - 1) * GS, GS)

    def rows_to(h, k):
        return pltpu.make_async_remote_copy(
            rc.at[side(k), part_of(h)], xrc.at[ti, part_of(h)], rcss.at[h, k], rcrs.at[h, k],
            device_id={"tensor": side(k)}, device_id_type=MESH,
        )

    def act_to(h, k):
        return pltpu.make_async_remote_copy(
            gact.at[part_of(h)], xact.at[ti, part_of(h)], actss.at[h, k], actrs.at[h, k],
            device_id={"tensor": side(k)}, device_id_type=MESH,
        )

    mine = pl.ds(pl.multiple_of(ti * DT, DT), DT)

    def down_to(k):
        return pltpu.make_async_remote_copy(
            down.at[side(k)], gd_ref.at[0, :, mine], dss.at[k], drs.at[k],
            device_id={"tensor": side(k)}, device_id_type=MESH,
        )

    unpack(0)
    unpack(1)
    for n in range(3):
        for k in range(2):
            gathered(n, k).wait_recv()
            pass_on(n, k).start()
    for g in range(2, NG - 1):
        unpack(g)
    rows_to(0, 1).start()
    rows_to(0, 3).start()
    for n in range(3):
        for k in range(2):
            passed_on(n, k).wait_recv()
    rows_to(0, 2).start()
    expert(0, NG - 1)
    for k in (1, 3, 2):
        act_to(0, k).start()
    unpack(NG - 1)
    for k in (1, 3, 2):
        rows_to(1, k).start()
    expert(NG - 1, NG)
    for k in (1, 3, 2):
        act_to(1, k).start()
    xrc[ti] = rc[ti]
    xact[ti] = gact[...]
    ret[0] = rsend[0]
    for h in range(2):
        for k in range(1, T):
            rows_to(h, k).wait_recv()
            act_to(h, k).wait_recv()
    CB = 256
    acts = xact[:, :, 2 * FF : 3 * FF].reshape(T * SL, FF)
    for n in range(DT // CB):
        r = xrc[:, :, DT + n * CB : DT + (n + 1) * CB].reshape(T * SL, CB)
        v = dot(acts, r, 0, 0).astype(BF)
        down[:, :, n * CB : (n + 1) * CB] = v.reshape(T, FT, CB)
    for k in (1, 3, 2):
        down_to(k).start()
    gd_ref[0, :, mine] = down[ti]
    acts = xact[:, :, 0 : 2 * FF].reshape(T * SL, 2 * FF)
    for n in range(DT // CB):
        r = xrc[:, :, n * CB : (n + 1) * CB].reshape(T * SL, CB)
        v = dot(r, acts, 0, 0).astype(BF)
        gg_ref[0, n * CB : (n + 1) * CB, :] = v[:, 0:FF]
        gu_ref[0, n * CB : (n + 1) * CB, :] = v[:, FF : 2 * FF]

    unpick = pick[...].astype(F32).T.astype(BF)

    def wait_back(j, c):
        back(j).wait_recv()
        return c

    def drain(j, c):
        dispatch(j).wait_send()
        back(j).wait_send()
        return c

    lax.fori_loop(1, E, drain, 0)
    for n in range(3):
        for k in range(2):
            gather(n, k).wait_send()
            pass_on(n, k).wait_send()
    for k in range(1, T):
        for h in range(2):
            rows_to(h, k).wait_send()
            act_to(h, k).wait_send()
        down_to(k).wait_send()
        down_to(k).wait_recv()
    lax.fori_loop(1, E, wait_back, 0)
    for n in range(DT // CB):
        r = ret[:, :, n * CB : (n + 1) * CB].reshape(E * ROWS, CB)
        v = dot(unpick, r).astype(BF)
        for q in range(T):
            ig_ref[:, q * DT + n * CB : q * DT + (n + 1) * CB] = v[q * TOK : (q + 1) * TOK]


def put(*refs):
    n = (len(refs) - 1) // 2
    copies = [pltpu.make_async_copy(refs[i], refs[n + i], refs[-1].at[i]) for i in range(n)]
    for c in copies:
        c.start()
    for c in copies:
        c.wait()


def local(tokens, cotangent, expert_ids, gate_wts, w_gate, w_up, w_down):
    TOK, D = tokens.shape
    E = lax.axis_size("expert")
    T = lax.axis_size("tensor")
    FF = w_gate.shape[2]
    CAP = 2 * TOK // E
    DT, FT, SL, ROWS = D // T, FF // T, E * CAP, T * CAP
    shapes = ((TOK, D), (1, DT, FF), (1, DT, FF), (1, FT, D))
    vm = pl.BlockSpec(memory_space=pltpu.VMEM)
    hb = pl.BlockSpec(memory_space=pl.ANY)
    dma = pltpu.SemaphoreType.DMA
    outs = pl.pallas_call(
        functools.partial(body, (E, T, CAP, TOK, D, FF)),
        name="routed_backward",
        out_shape=tuple(pltpu.VMEM(s, BF) for s in shapes),
        in_specs=[hb] * 7,
        out_specs=(vm, vm, vm, vm),
        scratch_shapes=[
            pltpu.VMEM((2, TOK), jnp.int32),
            pltpu.VMEM((2, TOK), F32),
            pltpu.VMEM((T * TOK, DT), BF),
            pltpu.VMEM((T * TOK, DT), BF),
            pltpu.VMEM((T, DT, FF), BF),
            pltpu.VMEM((T, DT, FF), BF),
            pltpu.VMEM((T, FT, D), BF),
            pltpu.VMEM((E * ROWS, T * TOK), BF),
            pltpu.VMEM((E, 2 * ROWS, DT), BF),
            pltpu.VMEM((E, 2 * ROWS, DT), BF),
            pltpu.VMEM((T, SL, 2 * DT), BF),
            pltpu.VMEM((SL, 3 * FF), BF),
            pltpu.VMEM((E, ROWS, DT), BF),
            pltpu.VMEM((E, ROWS, DT), BF),
            pltpu.VMEM((T, SL, 2 * DT), BF),
            pltpu.VMEM((T, SL, 3 * FF), BF),
            pltpu.VMEM((T, FT, DT), BF),
            pltpu.SemaphoreType.REGULAR((E // 4,)), pltpu.SemaphoreType.REGULAR((E // 4,)),
            dma((2 * T + 5,)),
            dma((E,)), dma((E,)),
            dma((3, 4)), dma((3, 4)),
            dma((E,)), dma((E,)),
            dma((2, T)), dma((2, T)),
            dma((2, T)), dma((2, T)),
            dma((T,)), dma((T,)),
        ],
        compiler_params=pltpu.CompilerParams(
            collective_id=0, has_side_effects=True, vmem_limit_bytes=56 << 20
        ),
    )(expert_ids.T, gate_wts.T, tokens, cotangent, w_gate, w_up, w_down)
    outs = [pltpu.with_memory_space_constraint(o, pltpu.VMEM) for o in outs]
    return pl.pallas_call(
        put,
        name="put",
        out_shape=tuple(jax.ShapeDtypeStruct(s, BF) for s in shapes),
        in_specs=[vm] * 4,
        out_specs=(hb,) * 4,
        scratch_shapes=[dma((4,))],
    )(*outs)


def solution(mesh):
    rows = P(("group", "expert", "tensor"), None)
    grads = P(("group", "expert"), "tensor", None)
    return jax.shard_map(
        local,
        mesh=mesh,
        in_specs=(rows, rows, rows, rows) + (P("expert", "tensor", None),) * 3,
        out_specs=(rows, grads, grads, grads),
        check_vma=False,
    )
```

```python
import functools

import jax
import jax.numpy as jnp
from jax import lax
from jax.experimental import pallas as pl
from jax.experimental.pallas import tpu as pltpu
from jax.sharding import PartitionSpec as P

BF = jnp.bfloat16
F32 = jnp.float32
MESH = pl.DeviceIdType.MESH


def dot(a, b, ca=1, cb=0):
    return lax.dot_general(a, b, (((ca,), (cb,)), ((), ())), preferred_element_type=F32)


def iota(shape, axis):
    return lax.broadcasted_iota(jnp.int32, shape, axis)


def body(
    sizes,
    ids_hbm, gts_hbm, tok_hbm, cot_hbm, wg_hbm, wu_hbm, wd_hbm,
    ret, unpick, gg_ref, gu_ref, gd_ref,
    idv, gtv, tokv, cotv, wg, wu, wd, pick, send, recv, rc, gact, rsend, xrc, xact, down,
    from_up, from_below, in_sem, ssem, rsem, wssem, wrsem, bssem, brsem, rcss, rcrs, actss, actrs, dss, drs,
):
    E, T, CAP, TOK, D, FF = sizes
    Z = E // 2
    DT = D // T
    FT = FF // T
    ROWS = T * CAP
    GRP = 8
    NG = E // GRP
    GS = GRP * CAP
    SL = E * CAP
    me = lax.axis_index("expert")
    ti = lax.axis_index("tensor")

    def partner(j, sign):
        u = j // 2
        near = (u + 1) // 2
        step = (u % 2) * near + (1 - u % 2) * (Z - near)
        away = step if sign > 0 else Z - step
        return ((me // 2 + away) % Z) * 2 + (me % 2 + j) % 2

    def side(k):
        return (ti + k) % T

    bar = pltpu.get_barrier_semaphore()
    z, core = me // 2, me % 2
    up, below = (z + 1) % Z, (z + Z - 1) % Z
    near_by = [z * 2 + 1 - core, up * 2 + core, up * 2 + 1 - core, below * 2 + core, below * 2 + 1 - core]
    for e in near_by:
        pl.semaphore_signal(bar, 1, device_id={"expert": e}, device_id_type=MESH)
    for k in (1, T - 1):
        pl.semaphore_signal(bar, 1, device_id={"tensor": side(k)}, device_id_type=MESH)

    def tell_up(k):
        pl.semaphore_signal(from_below.at[k], 1, device_id={"expert": up * 2 + core}, device_id_type=MESH)

    def tell_below(k):
        pl.semaphore_signal(from_up.at[k], 1, device_id={"expert": below * 2 + core}, device_id_type=MESH)

    loads = []

    def load(src, dst, k):
        c = pltpu.make_async_copy(src, dst, in_sem.at[k])
        c.start()
        return c

    head = [load(ids_hbm, idv, 2 * T + 3), load(gts_hbm, gtv, 2 * T + 4)]
    for q in range(T):
        loads.append(load(tok_hbm.at[:, pl.ds(q * DT, DT)], tokv.at[pl.ds(q * TOK, TOK)], q))
    for q in range(T):
        loads.append(load(cot_hbm.at[:, pl.ds(q * DT, DT)], cotv.at[pl.ds(q * TOK, TOK)], T + q))
    loads.append(load(wg_hbm.at[0], wg.at[ti], 2 * T))
    loads.append(load(wu_hbm.at[0], wu.at[ti], 2 * T + 1))
    loads.append(load(wd_hbm.at[0], wd.at[ti], 2 * T + 2))

    W = T * TOK
    for c in head:
        c.wait()
    i0 = idv[0:1, :]
    i1 = idv[1:2, :]
    ex = iota((E, TOK), 0)
    h0 = i0 == ex
    h1 = i1 == ex
    both = (jnp.where(h0, 1.0, 0.0) + jnp.where(h1, 1.0, 0.0)).astype(BF)
    before = jnp.where(iota((TOK, TOK), 0) < iota((TOK, TOK), 1), 1.0, 0.0).astype(BF)
    count = dot(both, before)
    p0 = jnp.sum(jnp.where(h0, count, 0.0), axis=0, keepdims=True).astype(jnp.int32)
    p1 = jnp.sum(jnp.where(h1, count, 0.0), axis=0, keepdims=True).astype(jnp.int32)

    def wide(v):
        return jnp.concatenate([v] * T, axis=1)

    s0 = wide(jnp.where(p0 < CAP, i0 * CAP + p0, -1))
    s1 = wide(jnp.where(p1 < CAP, i1 * CAP + p1, -1))
    g0 = wide(gtv[0:1, :])
    g1 = wide(gtv[1:2, :])

    for c in loads[: 2 * T]:
        c.wait()

    EB = 4
    RB = EB * ROWS

    def dispatch(j):
        return pltpu.make_async_remote_copy(
            send.at[j], recv.at[j], ssem.at[j], rsem.at[j],
            device_id={"expert": partner(j, 1)}, device_id_type=MESH,
        )

    def build(i):
        r = iota((RB, 1), 0) + i * RB
        j = r // ROWS
        u = j // 2
        near = (u + 1) // 2
        step = jnp.where(u % 2 == 1, near, Z - near)
        slot = (((z + step) % Z) * 2 + (core + j) % 2) * CAP + r % CAP
        same = (r // CAP) % T == iota((1, W), 1) // TOK
        m0 = (s0 == slot) & same
        m1 = (s1 == slot) & same
        o = jnp.where(m0 | m1, 1.0, 0.0).astype(BF)
        gate = jnp.sum(jnp.where(m0, g0, 0.0) + jnp.where(m1, g1, 0.0), axis=1, keepdims=True)
        pick[pl.ds(i * RB, RB), :] = o
        x = dot(o, tokv[...]).astype(BF)
        send[pl.ds(i * EB, EB), 0:ROWS, :] = x.reshape(EB, ROWS, DT)
        y = (gate * dot(o, cotv[...])).astype(BF)
        send[pl.ds(i * EB, EB), ROWS : 2 * ROWS, :] = y.reshape(EB, ROWS, DT)

    weights = (wg, wu, wd)

    def gather(n, k):
        return pltpu.make_async_remote_copy(
            weights[n].at[ti], weights[n].at[ti], wssem.at[n, k], wrsem.at[n, k],
            device_id={"tensor": side(1 if k == 0 else T - 1)}, device_id_type=MESH,
        )

    def gathered(n, k):
        src = side(T - 1 if k == 0 else 1)
        return pltpu.make_async_remote_copy(
            weights[n].at[src], weights[n].at[src], wssem.at[n, k], wrsem.at[n, k],
            device_id={"tensor": side(1)}, device_id_type=MESH,
        )

    def pass_on(n, k):
        h = weights[n].shape[1] // 2
        part = weights[n].at[side(T - 1 if k == 0 else 1), pl.ds(k * h, h)]
        return pltpu.make_async_remote_copy(
            part, part, wssem.at[n, 2 + k], wrsem.at[n, 2 + k],
            device_id={"tensor": side(1 if k == 0 else T - 1)}, device_id_type=MESH,
        )

    def passed_on(n, k):
        h = weights[n].shape[1] // 2
        part = weights[n].at[side(2), pl.ds(k * h, h)]
        return pltpu.make_async_remote_copy(
            part, part, wssem.at[n, 2 + k], wrsem.at[n, 2 + k],
            device_id={"tensor": side(1)}, device_id_type=MESH,
        )

    build(0)
    pl.semaphore_wait(bar, len(near_by) + 2)
    tell_below(1)
    tell_up(1)
    for j in range(1, EB):
        dispatch(j).start()
    for n in range(3):
        loads[2 * T + n].wait()
    for n in range(3):
        for k in range(2):
            gather(n, k).start()
    NC = E // EB

    def chunk(i, c):
        build(i)
        pl.semaphore_wait(from_up.at[i], 1)

        @pl.when(i < NC - 1)
        def _():
            tell_below(i + 1)

        @pl.when(i > 1)
        def _():
            pl.semaphore_wait(from_below.at[i - 1], 1)

            @pl.when(i < NC - 1)
            def _():
                tell_up(i)

        for j in range(EB):
            dispatch(i * EB + j).start()
        return c

    lax.fori_loop(1, NC, chunk, 0)
    recv[0] = send[0]

    MB = 2 * ROWS
    fo = iota((GRP * MB, GRP * MB), 0)
    fi = iota((GRP * MB, GRP * MB), 1)
    want = (((fo % GS) // CAP) * MB) + (fo // (T * GS)) * ROWS + ((fo // GS) % T) * CAP + fo % CAP
    spread = jnp.where(fi == want, 1.0, 0.0).astype(BF)
    bo = iota((GRP * ROWS, GRP * ROWS), 0)
    bi = iota((GRP * ROWS, GRP * ROWS), 1)
    wantb = ((bo // CAP) % T) * GS + (bo // ROWS) * CAP + bo % CAP
    fold = jnp.where(bi == wantb, 1.0, 0.0).astype(BF)

    def wait_dispatch(j, c):
        dispatch(j).wait_recv()
        return c

    def unpack(g):
        lax.fori_loop(max(1, g * GRP), (g + 1) * GRP, wait_dispatch, 0)
        for half in range(2):
            cols = pl.ds(half * (DT // 2), DT // 2)
            m = recv[pl.ds(g * GRP, GRP), :, cols].reshape(GRP * MB, DT // 2)
            v = dot(spread, m).astype(BF)
            for q in range(T):
                rc[q, pl.ds(g * GS, GS), cols] = v[q * GS : (q + 1) * GS]
                cols2 = pl.ds(DT + half * (DT // 2), DT // 2)
                rc[q, pl.ds(g * GS, GS), cols2] = v[(T + q) * GS : (T + q + 1) * GS]

    def back(j):
        to = partner(j, -1)
        return pltpu.make_async_remote_copy(
            rsend.at[j], ret.at[j], bssem.at[j], brsem.at[j],
            device_id={"expert": to}, device_id_type=MESH,
        )

    def start_back(j, last):
        back(last - j).start()
        return last

    def expert(lo, hi):
        sl = pl.ds(lo * GS, (hi - lo) * GS)
        pg = sum(dot(rc[q, sl, 0:DT], wg[q]) for q in range(T))
        pu = sum(dot(rc[q, sl, 0:DT], wu[q]) for q in range(T))
        gh = sum(
            dot(rc[q, sl, DT : 2 * DT], wd[:, :, q * DT : (q + 1) * DT].reshape(FF, DT), 1, 1)
            for q in range(T)
        )
        sg = jax.nn.sigmoid(pg)
        act = pg * sg
        gact[sl, 2 * FF : 3 * FF] = (act * pu).astype(BF)
        a = (gh * pu * sg * (1.0 + pg * (1.0 - sg))).astype(BF)
        b = (gh * act).astype(BF)
        gact[sl, 0:FF] = a
        gact[sl, FF : 2 * FF] = b
        parts = [(dot(a, wg[q], 1, 1) + dot(b, wu[q], 1, 1)).astype(BF) for q in range(T)]
        for g in range(lo, hi):
            o = (g - lo) * GS
            m = jnp.concatenate([p[o : o + GS] for p in parts], axis=0)
            v = dot(fold, m).astype(BF)
            rsend[pl.ds(g * GRP, GRP)] = v.reshape(GRP, ROWS, DT)
        lax.fori_loop(max(1, lo * GRP), hi * GRP, start_back, max(1, lo * GRP) + hi * GRP - 1)

    def part_of(h):
        return pl.ds(0, (NG - 1) * GS) if h == 0 else pl.ds((NG - 1) * GS, GS)

    def rows_to(h, k):
        return pltpu.make_async_remote_copy(
            rc.at[side(k), part_of(h)], xrc.at[ti, part_of(h)], rcss.at[h, k], rcrs.at[h, k],
            device_id={"tensor": side(k)}, device_id_type=MESH,
        )

    def act_to(h, k):
        return pltpu.make_async_remote_copy(
            gact.at[part_of(h)], xact.at[ti, part_of(h)], actss.at[h, k], actrs.at[h, k],
            device_id={"tensor": side(k)}, device_id_type=MESH,
        )

    mine = pl.ds(pl.multiple_of(ti * DT, DT), DT)

    def down_to(k):
        return pltpu.make_async_remote_copy(
            down.at[side(k)], gd_ref.at[0, :, mine], dss.at[k], drs.at[k],
            device_id={"tensor": side(k)}, device_id_type=MESH,
        )

    unpack(0)
    unpack(1)
    for n in range(3):
        for k in range(2):
            gathered(n, k).wait_recv()
            pass_on(n, k).start()
    for g in range(2, NG - 1):
        unpack(g)
    rows_to(0, 1).start()
    rows_to(0, 3).start()
    for n in range(3):
        for k in range(2):
            passed_on(n, k).wait_recv()
    rows_to(0, 2).start()
    expert(0, NG - 1)
    for k in (1, 3, 2):
        act_to(0, k).start()
    unpack(NG - 1)
    for k in (1, 3, 2):
        rows_to(1, k).start()
    expert(NG - 1, NG)
    for k in (1, 3, 2):
        act_to(1, k).start()
    xrc[ti] = rc[ti]
    xact[ti] = gact[...]
    ret[0] = rsend[0]
    for h in range(2):
        for k in range(1, T):
            rows_to(h, k).wait_recv()
            act_to(h, k).wait_recv()
    CB = 256
    acts = xact[:, :, 2 * FF : 3 * FF].reshape(T * SL, FF)
    for n in range(DT // CB):
        r = xrc[:, :, DT + n * CB : DT + (n + 1) * CB].reshape(T * SL, CB)
        v = dot(acts, r, 0, 0).astype(BF)
        down[:, :, n * CB : (n + 1) * CB] = v.reshape(T, FT, CB)
    for k in (1, 3, 2):
        down_to(k).start()
    gd_ref[0, :, mine] = down[ti]
    acts = xact[:, :, 0 : 2 * FF].reshape(T * SL, 2 * FF)
    for n in range(DT // CB):
        r = xrc[:, :, n * CB : (n + 1) * CB].reshape(T * SL, CB)
        v = dot(r, acts, 0, 0).astype(BF)
        gg_ref[0, n * CB : (n + 1) * CB, :] = v[:, 0:FF]
        gu_ref[0, n * CB : (n + 1) * CB, :] = v[:, FF : 2 * FF]

    unpick[...] = pick[...].astype(F32).T.astype(BF)

    def wait_back(j, c):
        back(j).wait_recv()
        return c

    def drain(j, c):
        dispatch(j).wait_send()
        back(j).wait_send()
        return c

    lax.fori_loop(1, E, drain, 0)
    for n in range(3):
        for k in range(2):
            gather(n, k).wait_send()
            pass_on(n, k).wait_send()
    for k in range(1, T):
        for h in range(2):
            rows_to(h, k).wait_send()
            act_to(h, k).wait_send()
        down_to(k).wait_send()
        down_to(k).wait_recv()
    lax.fori_loop(1, E, wait_back, 0)


def put(ret, unpick, gg, gu, gd, ig_out, gg_out, gu_out, gd_out, ig, sem):
    copies = [
        pltpu.make_async_copy(src, dst, sem.at[i])
        for i, (src, dst) in enumerate(((gg, gg_out), (gu, gu_out), (gd, gd_out)))
    ]
    for c in copies:
        c.start()
    TOK, D = ig.shape
    E, ROWS, DT = ret.shape
    T = D // DT
    for q in range(T):
        v = dot(unpick[q * TOK : (q + 1) * TOK, :], ret[...].reshape(E * ROWS, DT)).astype(BF)
        cols = pl.ds(q * DT, DT)
        ig[:, cols] = v
        c = pltpu.make_async_copy(ig.at[:, cols], ig_out.at[:, cols], sem.at[3 + q])
        c.start()
        copies.append(c)
    for c in copies:
        c.wait()


def local(tokens, cotangent, expert_ids, gate_wts, w_gate, w_up, w_down):
    TOK, D = tokens.shape
    E = lax.axis_size("expert")
    T = lax.axis_size("tensor")
    FF = w_gate.shape[2]
    CAP = 2 * TOK // E
    DT, FT, SL, ROWS = D // T, FF // T, E * CAP, T * CAP
    shapes = ((TOK, D), (1, DT, FF), (1, DT, FF), (1, FT, D))
    inner = ((E, ROWS, DT), (T * TOK, E * ROWS)) + shapes[1:]
    vm = pl.BlockSpec(memory_space=pltpu.VMEM)
    hb = pl.BlockSpec(memory_space=pl.ANY)
    dma = pltpu.SemaphoreType.DMA
    outs = pl.pallas_call(
        functools.partial(body, (E, T, CAP, TOK, D, FF)),
        name="routed_backward",
        out_shape=tuple(pltpu.VMEM(s, BF) for s in inner),
        in_specs=[hb] * 7,
        out_specs=(vm,) * 5,
        scratch_shapes=[
            pltpu.VMEM((2, TOK), jnp.int32),
            pltpu.VMEM((2, TOK), F32),
            pltpu.VMEM((T * TOK, DT), BF),
            pltpu.VMEM((T * TOK, DT), BF),
            pltpu.VMEM((T, DT, FF), BF),
            pltpu.VMEM((T, DT, FF), BF),
            pltpu.VMEM((T, FT, D), BF),
            pltpu.VMEM((E * ROWS, T * TOK), BF),
            pltpu.VMEM((E, 2 * ROWS, DT), BF),
            pltpu.VMEM((E, 2 * ROWS, DT), BF),
            pltpu.VMEM((T, SL, 2 * DT), BF),
            pltpu.VMEM((SL, 3 * FF), BF),
            pltpu.VMEM((E, ROWS, DT), BF),
            pltpu.VMEM((T, SL, 2 * DT), BF),
            pltpu.VMEM((T, SL, 3 * FF), BF),
            pltpu.VMEM((T, FT, DT), BF),
            pltpu.SemaphoreType.REGULAR((E // 4,)), pltpu.SemaphoreType.REGULAR((E // 4,)),
            dma((2 * T + 5,)),
            dma((E,)), dma((E,)),
            dma((3, 4)), dma((3, 4)),
            dma((E,)), dma((E,)),
            dma((2, T)), dma((2, T)),
            dma((2, T)), dma((2, T)),
            dma((T,)), dma((T,)),
        ],
        compiler_params=pltpu.CompilerParams(
            collective_id=0, has_side_effects=True, vmem_limit_bytes=56 << 20
        ),
    )(expert_ids.T, gate_wts.T, tokens, cotangent, w_gate, w_up, w_down)
    outs = [pltpu.with_memory_space_constraint(o, pltpu.VMEM) for o in outs]
    return pl.pallas_call(
        put,
        name="put",
        out_shape=tuple(jax.ShapeDtypeStruct(s, BF) for s in shapes),
        in_specs=[vm] * 5,
        out_specs=(hb,) * 4,
        scratch_shapes=[pltpu.VMEM((TOK, D), BF), dma((3 + T,))],
    )(*outs)


def solution(mesh):
    rows = P(("group", "expert", "tensor"), None)
    grads = P(("group", "expert"), "tensor", None)
    return jax.shard_map(
        local,
        mesh=mesh,
        in_specs=(rows, rows, rows, rows) + (P("expert", "tensor", None),) * 3,
        out_specs=(rows, grads, grads, grads),
        check_vma=False,
    )
```
